256 devices in a mesh: user: 64 (over z, x, core), pos: 4 (over y).
Axes of the slice: x: 4, y: 4, z: 8, core: 2. Of those that a mesh axis runs over, the one named last changes fastest.
Arguments:
- events: bfloat16 [65536, 256], P('user'), may hold values from -6 to 6
- owners: int32 [65536], P('user'), may hold values from 0 to 127, as said below
- offsets: int32 [65536], P('user'), may hold values from 0 to 2047, as said below
- w_key: bfloat16 [256, 256], replicated, may hold values from -0.375 to 0.375
- w_value: bfloat16 [256, 256], replicated, may hold values from -0.375 to 0.375
- cache_keys: bfloat16 [128, 6144, 256], P('user', 'pos'), may hold values from -7 to 7
- cache_values: bfloat16 [128, 6144, 256], P('user', 'pos'), may hold values from -6 to 6
- hist_len: int32 [128], P('user'), may hold values from 8 to 4096
- active: int32 [128], P('user'), may hold values 0 or 1
- candidates: bfloat16 [128, 1024, 256], P('user', 'pos'), may hold values from -100 to 100
Outputs:
- new_keys: bfloat16 [128, 6144, 256], P('user', 'pos')
- new_values: bfloat16 [128, 6144, 256], P('user', 'pos')
- attended: bfloat16 [128, 1024, 256], P('user', 'pos')
The draws below stay inside these ranges and needn't reach their ends.
Inputs may be any that keep to these rules, and one draw needn't show every extreme that they name: Among the events of one aligned block of 1024 (one index of user), at most 32 have owners among the users t * 2 to t * 2 + 1, for every t; in every draw some t receives exactly 32 from every block, and all those events belong to one user of that t. offsets[e] is the number of events before e, in the order of the array, that have the same owner as e.
All inputs are finite; a program needn't handle non-finite values. No bound on the sum of `active` on one device may be relied on, other than what follows from the above.
Results may differ from the reference program's by a relative error of at most 0.0067.
Values may be sent and summed in bfloat16 or wider, within the bound.
No kernel may reach another device: no remote copies, remote signals or barrier semaphores. Data moves between devices by JAX's collectives and lax.ppermute only.
A program may use at most 128 MiB of HBM per device.

```python
import jax
import jax.numpy as jnp
from jax import lax

U_DEV = 2
P_DEV = 1536
EV_DEV = 1024
D = 256
F = 256
CAND = 1024
USERS = 128
HIST = 6144
EVENTS = 65536
CAP = 32
N_POS = 4


def key_head(key):
    head = jnp.clip(jax.random.normal(jax.random.fold_in(key, 7002), (USERS, 6, D), jnp.float32), -6.0, 6.0)
    return head


def draw_cache_keys(key, part):
    rows = jnp.clip(jax.random.normal(jax.random.fold_in(key, 7001), (USERS, HIST, D), jnp.float32), -6.0, 6.0)
    head = key_head(key)
    rows = rows.at[:, :6].set(head)
    return rows.astype(jnp.bfloat16)


def draw_candidates(key, part):
    values = jnp.clip(jax.random.normal(jax.random.fold_in(key, 7003), (USERS, CAND, D), jnp.float32), -6.0, 6.0)
    return values.astype(jnp.bfloat16)


def routing(key):
    groups = USERS // U_DEV
    width = groups * CAP
    splits = jax.random.split(jax.random.fold_in(key, 7101), groups)

    def shuffle(single):
        return jax.random.permutation(single, width).astype(jnp.int32)
    perms = jax.vmap(shuffle)(splits)
    full = jax.random.randint(jax.random.fold_in(key, 7102), (), 0, groups).astype(jnp.int32)
    column = jnp.arange(width, dtype=jnp.int32) // CAP
    score = jnp.where(column[None, :] == full, perms - width, perms)
    chosen = jnp.argsort(score, axis=1)[:, :EV_DEV].astype(jnp.int32)
    dest = chosen // CAP
    local = jax.random.randint(jax.random.fold_in(key, 7103), (groups, EV_DEV), 0, U_DEV).astype(jnp.int32)
    heavy = jax.random.randint(jax.random.fold_in(key, 7104), (), 0, U_DEV).astype(jnp.int32)
    local = jnp.where(dest == full, heavy, local).astype(jnp.int32)
    owners = (dest * U_DEV + local).reshape(-1).astype(jnp.int32)
    order_all = jnp.argsort(owners, stable=True).astype(jnp.int32)
    sorted_owner = owners[order_all]
    start = jnp.searchsorted(sorted_owner, sorted_owner, side='left').astype(jnp.int32)
    rank_sorted = jnp.arange(EVENTS, dtype=jnp.int32) - start
    offsets = jnp.zeros((EVENTS,), jnp.int32).at[order_all].set(rank_sorted)
    return (owners, offsets)


def draw_owners(key, part):
    return routing(key)[0]


def draw_offsets(key, part):
    return routing(key)[1]


def touch_ends(result, key, low, top_value):
    longest = result.shape.index(max(result.shape))
    spots = []
    for shift in (0, 1):
        where = [jax.random.randint(jax.random.fold_in(key, axis), (), 0, length) for axis, length in enumerate(result.shape)]
        where[longest] = (where[longest] + shift) % result.shape[longest]
        spots.append(tuple(where))
    return result.at[spots[0]].set(low).at[spots[1]].set(top_value)


def block_scale(rng, extent, cuts, low, top_value):
    def one(dim, blocks):
        steps = jax.random.uniform(jax.random.fold_in(jax.random.fold_in(rng, 6), dim), (blocks,), jnp.float32, low / len(cuts), top_value / len(cuts))
        return jnp.repeat(jnp.exp(steps), extent[dim] // blocks).reshape((-1,) + (1,) * (len(extent) - dim - 1))

    loudness = one(*cuts[0])
    for cut in cuts[1:]:
        loudness = loudness * one(*cut)
    return loudness


def normal_values(rng, extent, spread, limit, pieces=(), kind=jnp.bfloat16):
    loudness = block_scale(rng, extent, pieces, -0.22, 0.18) if pieces else 1.0
    values = jax.random.normal(rng, extent, jnp.float32) * spread * loudness
    return jnp.minimum(jnp.maximum(values, -limit), limit).astype(kind)


def setup_inputs(seed: int = 0) -> dict:
    key_list = jax.random.split(jax.random.key(seed), 11)
    return {
        "events": normal_values(key_list[0], (EVENTS, F), 1.0, 6.0, ((0, 64),)),
        "owners": draw_owners(jax.random.fold_in(key_list[10], 71), 0),
        "offsets": draw_offsets(jax.random.fold_in(key_list[10], 71), 0),
        "w_key": normal_values(key_list[3], (F, D), F ** -0.5, 0.375),
        "w_value": normal_values(key_list[4], (F, D), F ** -0.5, 0.375),
        "cache_keys": draw_cache_keys(jax.random.fold_in(key_list[10], 71), 0),
        "cache_values": normal_values(key_list[6], (USERS, HIST, D), 1.0, 6.0, ((0, 64), (1, 4))),
        "hist_len": touch_ends(jax.random.randint(key_list[7], (USERS,), 8, HIST - 2 * EV_DEV + 1), jax.random.fold_in(key_list[7], 1), 8, HIST - 2 * EV_DEV).astype(jnp.int32),
        "active": touch_ends((jax.random.randint(key_list[8], (USERS,), 0, 4) < 3).astype(jnp.int32), jax.random.fold_in(key_list[8], 1), 0, 1),
        "candidates": draw_candidates(jax.random.fold_in(key_list[10], 71), 0),
    }


def reference(events, owners, offsets, w_key, w_value, cache_keys, cache_values, hist_len, active, candidates):
    new_k = jnp.dot(events, w_key, preferred_element_type=jnp.float32).astype(jnp.bfloat16)
    new_v = jnp.dot(events, w_value, preferred_element_type=jnp.float32).astype(jnp.bfloat16)
    target = (hist_len[owners] + offsets).astype(jnp.int32)
    new_keys = cache_keys.at[owners, target].set(new_k)
    new_values = cache_values.at[owners, target].set(new_v)
    counts = jax.ops.segment_sum(jnp.ones_like(owners), owners, num_segments=USERS).astype(jnp.int32)
    limits = (hist_len + counts).astype(jnp.int32)
    scale = D ** -0.5

    def per_user(pack):
        query, key_rows, value_rows, bound, flag = pack
        scores = jnp.dot(query, key_rows.T, preferred_element_type=jnp.float32) * scale
        scores = scores.reshape(CAND, N_POS, P_DEV)
        position = jnp.arange(HIST, dtype=jnp.int32).reshape(N_POS, P_DEV)
        valid = (position < bound)[None]
        masked = jnp.where(valid, scores, jnp.float32(-1e30))
        block_max = jnp.max(masked, axis=2)
        expo = jnp.where(valid, jnp.exp(masked - block_max[:, :, None]), jnp.float32(0.0))
        block_sum = jnp.sum(expo, axis=2)
        weights = expo.astype(jnp.bfloat16)
        parts = jnp.einsum("cbp,bpd->cbd", weights.astype(jnp.float32),
                           value_rows.reshape(N_POS, P_DEV, D).astype(jnp.float32))
        top = jnp.max(block_max, axis=1)
        factor = jnp.exp(block_max - top[:, None])
        total = jnp.sum(block_sum * factor, axis=1)
        acc = jnp.sum(parts * factor[:, :, None], axis=1)
        return (acc / total[:, None] * flag).astype(jnp.bfloat16)

    attended = lax.map(per_user, (candidates, new_keys, new_values, limits, active.astype(jnp.float32)))
    return new_keys, new_values, attended
```

```python
import jax
import jax.numpy as jnp
from jax import lax
from jax.experimental import pallas as pl
from jax.experimental.pallas import tpu as pltpu
from jax.sharding import PartitionSpec as P

NEG = -1e30
LOG2E = 1.4426950408889634
bf16 = jnp.bfloat16
f32 = jnp.float32
i32 = jnp.int32
NT = (((1,), (1,)), ((), ()))
ROW = 256
META = 128


def iota(shape, dim):
    return lax.broadcasted_iota(i32, shape, dim)


def split3(x):
    hi = x.astype(bf16)
    rest = x - hi.astype(f32)
    mid = rest.astype(bf16)
    low = (rest - mid.astype(f32)).astype(bf16)
    return hi, mid, low


def route_kernel(cap, groups):
    pieces = cap // 8

    def body(owners, offsets, events, out):
        n = owners.shape[1]
        users = 2 * groups
        own = owners[...]
        off = offsets[...]
        who = iota((users, n), 0)
        mine = who == own
        base = jnp.min(jnp.where(mine, off, jnp.int32(1 << 24)), axis=1, keepdims=True)
        count = jnp.sum(jnp.where(mine, 1.0, 0.0), axis=1, keepdims=True).astype(i32)
        odd = own % 2
        before = (who == own - 1) & (odd == 1)
        shift = jnp.where(mine, -base, 0) + jnp.where(before, count, 0)
        key = (own // 2) * cap + off + jnp.sum(shift, axis=0, keepdims=True)
        rows = groups * 8
        at = iota((rows, 1), 0)
        start = (at // 8) * cap + at % 8
        raw = events[...]
        for c in range(pieces):
            pick = jnp.where(start + 8 * c == key, 1.0, 0.0).astype(bf16)
            got = jnp.dot(pick, raw, preferred_element_type=f32)
            out[:, :, c * ROW : (c + 1) * ROW] = got.astype(bf16).reshape(groups, 8, ROW)
        ones = jnp.ones((n, META), bf16)
        first = jnp.where((at // 8) * 2 == own, 1.0, 0.0).astype(bf16)
        second = jnp.where((at // 8) * 2 + 1 == own, 1.0, 0.0).astype(bf16)
        c0 = jnp.dot(first, ones, preferred_element_type=f32)
        c1 = jnp.dot(second, ones, preferred_element_type=f32)
        both = jnp.where(iota((rows, META), 1) < META // 2, c0, c1)
        out[:, :, pieces * ROW :] = both.astype(bf16).reshape(groups, 8, META)

    return body


def old_kernel(span, scale):
    def body(info, q0, q1, q2, q3, keys, values, r0, r1, r2, r3):
        factor = scale * LOG2E
        users = keys.shape[0]
        cands = q0.shape[1]
        width = keys.shape[2]
        for q, r in ((q1, r1), (q3, r3), (q2, r2), (q0, r0)):
            marks = []
            for u in range(users):
                limit = info[u]
                s = lax.dot_general(q[u], keys[u], NT, preferred_element_type=f32)
                ok = iota((1, span), 1) < limit
                s = jnp.where(ok, s, NEG)
                top = jnp.max(s, axis=1, keepdims=True)
                e = jnp.exp2((s - top) * factor)
                some = (limit > 0).astype(f32)
                total = jnp.sum(e, axis=1, keepdims=True) * some
                part = jnp.dot(e.astype(bf16), values[u], preferred_element_type=f32) * some
                r[u * cands : (u + 1) * cands, :] = part.astype(bf16)
                marks += [top, total]
            lane = iota((cands, 128), 1)
            mat = jnp.zeros((cands, 128), f32)
            for i, v in enumerate(marks):
                mat = jnp.where(lane == i, v, mat)
            rows = mat.T[:8, :]
            hi, mid, low = split3(rows)
            pad = jnp.zeros_like(hi)
            r[users * cands :, :] = jnp.concatenate([hi, mid, low, pad], axis=0)

    return body


GUARD = 64


def new_kernel(cap, groups, span, scale):
    pieces = cap // 8
    slots = groups * 8

    def body(
        info, rows, w, q, r0, r1, r2, r3, keys, values, nk, nv, att,
        flat, place_k, place_v, table, table_s, sem,
    ):
        factor = scale * LOG2E
        users = q.shape[0]
        cands = q.shape[1]
        width = q.shape[2]
        meta = rows[:, :, pieces * ROW :].reshape(slots, META)
        src = iota((groups, slots), 0)
        col = iota((groups, slots), 1)
        lead = (col % 8) == 0
        earlier = jnp.where(lead & (col // 8 < src), 1.0, 0.0).astype(bf16)
        same = jnp.where(lead & (col // 8 == src), 1.0, 0.0).astype(bf16)
        begin = jnp.dot(earlier, meta, preferred_element_type=f32)
        here = jnp.dot(same, meta, preferred_element_type=f32)
        lane = iota((groups, META), 1)
        table[...] = jnp.where(lane % 2 == 0, begin, here).astype(i32)
        send = pltpu.make_async_copy(table, table_s, sem)
        send.start()

        kvs = []
        for c in range(pieces):
            x = rows[:, :, c * ROW : (c + 1) * ROW].reshape(slots, ROW)
            y = jnp.dot(x, w[...], preferred_element_type=f32).astype(bf16)
            flat[c * slots : (c + 1) * slots, :] = y.astype(f32)
            kvs.append(y)

        mt = meta.astype(f32).T
        c0 = mt[0:1, :].astype(i32)
        c1 = mt[META // 2 : META // 2 + 1, :].astype(i32)
        at = iota((1, slots), 1) % 8
        send.wait()

        def put(s, carry):
            n0 = table_s[s, 1]
            for u in range(users):
                n = table_s[s, u * (META // 2) + 1]
                d = info[u] + table_s[s, u * (META // 2)]
                a = 0 if u == 0 else n0

                @pl.when((n > 0) & (d < span) & (d + n > 0))
                def _():
                    for c in range(pieces):
                        slot = iota((8, 128), 0) + 8 * c
                        ok = (slot >= a) & (slot < a + n)
                        to = d - a + 8 * c + GUARD
                        from_row = pl.multiple_of(c * slots + s * 8, 8)
                        for j in range(width // 128):
                            for dst, o in ((place_k, 0), (place_v, width)):
                                v = flat[pl.ds(from_row, 8), o + j * 128 : o + (j + 1) * 128]
                                pltpu.store(dst.at[u, j, pl.ds(to, 8), :], v, mask=ok)
            return carry

        lax.fori_loop(0, groups, put, 0)

        for u in range(users):
            first = info[u]
            count = table_s[groups - 1, u * (META // 2)] + table_s[groups - 1, u * (META // 2) + 1]
            last = first + count
            step = 256
            for b in range(span // step):
                hit = (first < (b + 1) * step) & (last > b * step) & (count > 0)
                at_rows = iota((step, 128), 0) + b * step
                for src_ref, old, out in ((place_k, keys, nk), (place_v, values, nv)):

                    @pl.when(hit)
                    def _():
                        ok = (at_rows >= first) & (at_rows < last)
                        for j in range(width // 128):
                            new = src_ref[u, j, GUARD + b * step : GUARD + (b + 1) * step, :]
                            was = old[u, b * step : (b + 1) * step, j * 128 : (j + 1) * 128]
                            out[u, b * step : (b + 1) * step, j * 128 : (j + 1) * 128] = jnp.where(
                                ok, new, was.astype(f32)
                            ).astype(bf16)

                    @pl.when(jnp.logical_not(hit))
                    def _():
                        out[u, b * step : (b + 1) * step, :] = old[u, b * step : (b + 1) * step, :]

        k_all = jnp.concatenate([y[:, :width] for y in kvs], axis=0)
        v_all = jnp.concatenate([y[:, width:] for y in kvs], axis=0)
        parts = (r0, r1, r2, r3)
        marks = []
        for r in parts:
            m = r[users * cands :, :].astype(f32)
            marks.append(m[0:8] + m[8:16] + m[16:24])
        for u in range(users):
            oks = []
            for c in range(pieces):
                slot = at + 8 * c
                oks.append(slot < c0 if u == 0 else (slot >= c0) & (slot < c0 + c1))
            ok = jnp.concatenate([o.astype(i32) for o in oks], axis=1) > 0
            s = lax.dot_general(q[u], k_all, NT, preferred_element_type=f32)
            s = jnp.where(ok, s, NEG)
            top_new = jnp.max(s, axis=1, keepdims=True)
            tops = jnp.concatenate([m[2 * u : 2 * u + 1] for m in marks], axis=0)
            sums = jnp.concatenate([m[2 * u + 1 : 2 * u + 2] for m in marks], axis=0)
            cols = jnp.concatenate([tops, sums, jnp.zeros((120, cands), f32)], axis=0).T
            top_old = jnp.max(tops, axis=0, keepdims=True)
            top_old = jnp.max(cols[:, 0:4], axis=1, keepdims=True)
            top = jnp.maximum(top_new, top_old)
            e = jnp.where(ok, jnp.exp2((s - top) * factor), 0.0)
            total = jnp.sum(e, axis=1, keepdims=True)
            acc = jnp.dot(e.astype(bf16), v_all, preferred_element_type=f32)
            for i, r in enumerate(parts):
                g = jnp.exp2((cols[:, i : i + 1] - top) * factor)
                total = total + cols[:, 4 + i : 5 + i] * g
                acc = acc + r[u * cands : (u + 1) * cands, :].astype(f32) * g
            live = info[users + u].astype(f32)
            att[u] = (acc / total * live).astype(bf16)

    return body


def on_device(
    events, owners, offsets, w_key, w_value, cache_keys, cache_values, hist_len, active, candidates
):
    groups = lax.axis_size("user")
    blocks = lax.axis_size("pos")
    users = cache_keys.shape[0]
    span = cache_keys.shape[1]
    width = cache_keys.shape[2]
    cands = candidates.shape[1]
    per_event = events.shape[0]
    cap = 2 * per_event // groups
    scale = width ** (-0.5)
    here = lax.axis_index("pos")
    VM = pl.BlockSpec(memory_space=pltpu.VMEM)
    SM = pl.BlockSpec(memory_space=pltpu.SMEM)

    def moved(x, by):
        return lax.ppermute(x, "pos", [(i, (i + by) % blocks) for i in range(blocks)])

    q1 = moved(candidates, 1)
    q3 = moved(candidates, 3)
    q2 = moved(candidates, 2)

    wide = cap // 8 * ROW + META
    sent = pl.pallas_call(
        route_kernel(cap, groups),
        out_shape=jax.ShapeDtypeStruct((groups, 8, wide), bf16),
        in_specs=[VM] * 3,
        out_specs=VM,
        name="route",
    )(owners.reshape(1, -1), offsets.reshape(1, -1), events)
    rows = lax.all_to_all(sent, "user", split_axis=0, concat_axis=0, tiled=True)

    info = jnp.concatenate([hist_len - here * span, active]).astype(i32)
    r0, r1, r2, r3 = pl.pallas_call(
        old_kernel(span, scale),
        out_shape=[jax.ShapeDtypeStruct((users * cands + 32, width), bf16)] * 4,
        in_specs=[SM] + [VM] * 6,
        out_specs=[VM] * 4,
        name="old",
    )(info, candidates, q1, q2, q3, cache_keys, cache_values)
    b1 = moved(r1, blocks - 1)
    b3 = moved(r3, blocks - 3)
    b2 = moved(r2, blocks - 2)

    w = jnp.concatenate([w_key, w_value], axis=1)
    nk, nv, att = pl.pallas_call(
        new_kernel(cap, groups, span, scale),
        out_shape=[
            jax.ShapeDtypeStruct(cache_keys.shape, bf16),
            jax.ShapeDtypeStruct(cache_values.shape, bf16),
            jax.ShapeDtypeStruct(candidates.shape, bf16),
        ],
        in_specs=[SM] + [VM] * 9,
        out_specs=[VM] * 3,
        scratch_shapes=[
            pltpu.VMEM((cap * groups, 2 * width), f32),
            pltpu.VMEM((users, width // 128, GUARD + span + 32, 128), f32),
            pltpu.VMEM((users, width // 128, GUARD + span + 32, 128), f32),
            pltpu.VMEM((groups, META), i32),
            pltpu.SMEM((groups, META), i32),
            pltpu.SemaphoreType.DMA,
        ],
        name="new",
    )(info, rows, w, candidates, r0, b1, b2, b3, cache_keys, cache_values)
    return nk, nv, att


def solution(mesh):
    placed = (
        P("user", None),
        P("user"),
        P("user"),
        P(),
        P(),
        P("user", "pos", None),
        P("user", "pos", None),
        P("user"),
        P("user"),
        P("user", "pos", None),
    )
    return jax.shard_map(
        on_device,
        mesh=mesh,
        in_specs=placed,
        out_specs=(P("user", "pos", None), P("user", "pos", None), P("user", "pos", None)),
        check_vma=False,
    )
```

```python
import jax
import jax.numpy as jnp
from jax import lax
from jax.experimental import pallas as pl
from jax.experimental.pallas import tpu as pltpu
from jax.sharding import PartitionSpec as P


NEG = -1e30
LOG2E = 1.4426950408889634
bf16 = jnp.bfloat16
f32 = jnp.float32
i32 = jnp.int32
NT = (((1,), (1,)), ((), ()))
ROW = 256
META = 128
HALF = META // 2
GUARD = 64
STEP = 256


def iota(shape, dim):
    return lax.broadcasted_iota(i32, shape, dim)


def split3(x):
    hi = x.astype(bf16)
    rest = x - hi.astype(f32)
    mid = rest.astype(bf16)
    low = (rest - mid.astype(f32)).astype(bf16)
    return hi, mid, low


def fetch(pairs, sems):
    copies = [pltpu.make_async_copy(a, b, sems.at[i]) for i, (a, b) in enumerate(pairs)]
    for copy in copies:
        copy.start()
    return copies


def route_kernel(cap, groups, parts):
    pieces = cap // 8 // parts

    def body(owners_hbm, offsets_hbm, events_hbm, out, owners, offsets, events, sems):
        loads = fetch(((owners_hbm, owners), (offsets_hbm, offsets), (events_hbm, events)), sems)
        part = lax.axis_index("pos") % parts
        n = owners.shape[1]
        users = 2 * groups
        rows = groups * 8
        at = iota((rows, 1), 0)
        pair = (at // 8) * 2
        ones = jnp.ones((n, META), bf16)
        loads[0].wait()
        own = owners[...]
        first = jnp.where(pair == own, 1.0, 0.0).astype(bf16)
        second = jnp.where(pair + 1 == own, 1.0, 0.0).astype(bf16)
        c0 = jnp.dot(first, ones, preferred_element_type=f32)
        c1 = jnp.dot(second, ones, preferred_element_type=f32)
        both = jnp.where(iota((rows, META), 1) < HALF, c0, c1)
        out[:, :, pieces * ROW :] = both.astype(bf16).reshape(groups, 8, META)
        loads[1].wait()
        off = offsets[...]
        who = iota((users, n), 0)
        mine = who == own
        base = jnp.min(jnp.where(mine, off, jnp.int32(1 << 24)), axis=1, keepdims=True)
        count = jnp.sum(jnp.where(mine, 1.0, 0.0), axis=1, keepdims=True).astype(i32)
        before = (who == own - 1) & (own % 2 == 1)
        shift = jnp.where(mine, -base, 0) + jnp.where(before, count, 0)
        key = (own // 2) * cap + off + jnp.sum(shift, axis=0, keepdims=True)
        key = key - part * (cap // parts)
        start = (at // 8) * cap + at % 8
        loads[2].wait()
        raw = events[...]
        for c in range(pieces):
            pick = jnp.where(start + 8 * c == key, 1.0, 0.0).astype(bf16)
            got = jnp.dot(pick, raw, preferred_element_type=f32)
            out[:, :, c * ROW : (c + 1) * ROW] = got.astype(bf16).reshape(groups, 8, ROW)

    return body


def old_kernel(span, scale, chunks, keep):
    def body(hist, *refs):
        qs = refs[:chunks]
        refs = refs[chunks:]
        if keep:
            wk, wv, keys_hbm, values_hbm = refs[:4]
            outs = refs[4 : 4 + chunks]
            w, nk, nv, keys, values, sems, out_sems = refs[4 + chunks :]
        else:
            keys_hbm, values_hbm = refs[:2]
            outs = refs[2 : 2 + chunks]
            keys, values, sems = refs[2 + chunks :]
        users, cands, width = qs[0].shape
        loads = fetch(
            [p for u in range(users) for p in ((keys_hbm.at[u], keys.at[u]), (values_hbm.at[u], values.at[u]))],
            sems,
        )
        factor = scale * LOG2E
        base = lax.axis_index("pos") * span
        if keep:
            w[:, :width] = wk[...]
            w[:, width:] = wv[...]
        stores = []
        for i, (q, r) in enumerate(zip(qs, outs)):
            marks = []
            for u in range(users):
                if i == 0:
                    loads[2 * u].wait()
                    loads[2 * u + 1].wait()
                    if keep:
                        stores += fetch(
                            ((keys.at[u], nk.at[u]), (values.at[u], nv.at[u])), out_sems.at[u]
                        )
                s = lax.dot_general(q[u], keys[u], NT, preferred_element_type=f32)
                s = jnp.where(iota((1, span), 1) < hist[u] - base, s, NEG)
                top = jnp.max(s, axis=1, keepdims=True)
                e = jnp.exp2((s - top) * factor)
                total = jnp.sum(e, axis=1, keepdims=True)
                part = jnp.dot(e.astype(bf16), values[u], preferred_element_type=f32)
                r[u * cands : (u + 1) * cands, :] = part.astype(bf16)
                marks += [top, total]
            lane = iota((cands, 128), 1)
            mat = jnp.zeros((cands, 128), f32)
            for k, v in enumerate(marks):
                mat = jnp.where(lane == k, v, mat)
            rows = mat.T[:8, :]
            hi, mid, low = split3(rows)
            r[users * cands :, :] = jnp.concatenate([hi, mid, low, jnp.zeros_like(hi)], axis=0)
        for copy in stores:
            copy.wait()

    return body


def tables(meta, groups, slots):
    src = iota((groups, slots), 0)
    col = iota((groups, slots), 1)
    lead = (col % 8) == 0
    earlier = jnp.where(lead & (col // 8 < src), 1.0, 0.0).astype(bf16)
    same = jnp.where(lead & (col // 8 == src), 1.0, 0.0).astype(bf16)
    begin = jnp.dot(earlier, meta, preferred_element_type=f32)
    here = jnp.dot(same, meta, preferred_element_type=f32)
    lane = iota((groups, META), 1)
    return jnp.where(lane % 2 == 0, begin, here).astype(i32)


def project(refs, w, flat, slots):
    ys = []
    for c, (ref, lane) in enumerate(refs):
        x = ref[:, :, lane : lane + ROW].reshape(slots, ROW)
        y = jnp.dot(x, w[...], preferred_element_type=f32).astype(bf16)
        flat[c * slots : (c + 1) * slots, :] = y.astype(f32)
        ys.append(y)
    width = w.shape[1] // 2
    keys = jnp.concatenate([y[:, :width] for y in ys], axis=0)
    values = jnp.concatenate([y[:, width:] for y in ys], axis=0)
    return keys, values


def put_rows(hist, base, table_s, flat, place_k, place_v, base_slot, pieces, slots, groups, span):
    users = place_k.shape[0]
    tiles = place_k.shape[1]
    most = GUARD + span

    def put(s, carry):
        n0 = table_s[s, 1]
        for u in range(users):
            n = table_s[s, u * HALF + 1]
            d = hist[u] - base + table_s[s, u * HALF]
            a = 0 if u == 0 else n0
            for c in range(pieces):
                slot = iota((8, 128), 0) + (8 * c + base_slot)
                ok = (slot >= a) & (slot < a + n)
                to = jnp.clip(d - a + (8 * c + base_slot + GUARD), 0, most)
                from_row = pl.multiple_of(c * slots + s * 8, 8)
                for j in range(tiles):
                    for dst, o in ((place_k, 0), (place_v, tiles * 128)):
                        v = flat[pl.ds(from_row, 8), o + j * 128 : o + (j + 1) * 128]
                        pltpu.store(dst.at[u, j, pl.ds(to, 8), :], v, mask=ok)
        return carry

    lax.fori_loop(0, groups, put, 0, unroll=2)


def slot_ends(meta, pieces):
    mt = meta.astype(f32).T
    c0 = mt[0:1, :].astype(i32)
    c1 = mt[HALF : HALF + 1, :].astype(i32)
    end0 = jnp.concatenate([c0] * pieces, axis=1)
    end1 = jnp.concatenate([c0 + c1] * pieces, axis=1)
    return end0, end1


def new_scores(ends, base_slot, pieces, slots, q, keys):
    users, cands, width = q.shape
    end0, end1 = ends
    at = iota((1, slots), 1) % 8 + base_slot
    slot = jnp.concatenate([at + 8 * c for c in range(pieces)], axis=1)
    s = lax.dot_general(
        q[...].reshape(users * cands, width), keys, NT, preferred_element_type=f32
    )
    return jnp.concatenate(
        [
            jnp.where(slot < end0, s[:cands], NEG),
            jnp.where((slot >= end0) & (slot < end1), s[cands:], NEG),
        ],
        axis=0,
    )


def old_marks(olds, users, cands):
    marks = []
    for r in olds:
        m = r[users * cands :, :].astype(f32)
        marks.append(m[0:8] + m[8:16] + m[16:24])
    count = len(olds)
    stack = jnp.concatenate(
        [m[k : k + 1] for k in range(2 * users) for m in marks]
        + [jnp.zeros((128 - 2 * users * count, cands), f32)],
        axis=0,
    ).T
    per = 2 * count
    tops = jnp.concatenate([stack[:, per * u : per * u + count] for u in range(users)], axis=0)
    sums = jnp.concatenate(
        [stack[:, per * u + count : per * u + per] for u in range(users)], axis=0
    )
    return tops, sums


def bounds(hist, base, table_s, groups, u):
    first = hist[u] - base
    count = table_s[groups - 1, u * HALF] + table_s[groups - 1, u * HALF + 1]
    return first, first + count


def near_kernel(cap, groups, span, scale, parts):
    pieces = cap // 8 // parts
    slots = groups * 8

    def body(
        hist, rows, w, q, r0, r1, r3,
        place_k, place_v, acc_out, marks_out, table, ends_out,
        flat, table_s, sem,
    ):
        factor = scale * LOG2E
        users, cands, _ = q.shape
        here = lax.axis_index("pos")
        base = here * span
        base_slot = (here % parts) * (cap // parts)
        meta = rows[:, :, pieces * ROW :].reshape(slots, META)
        table[...] = tables(meta, groups, slots)
        send = pltpu.make_async_copy(table, table_s, sem)
        send.start()
        new_k, new_v = project([(rows, c * ROW) for c in range(pieces)], w, flat, slots)
        ends = slot_ends(meta, pieces)
        for i, row in enumerate(ends):
            ends_out[8 * i : 8 * i + 8, :] = jnp.broadcast_to(row, (8, pieces * slots))
        s = new_scores(ends, base_slot, pieces, slots, q, new_k)
        olds = (r0, r1, r3)
        tops, sums = old_marks(olds, users, cands)
        top = jnp.maximum(
            jnp.max(s, axis=1, keepdims=True), jnp.max(tops, axis=1, keepdims=True)
        )
        e = jnp.exp2((s - top) * factor)
        total = jnp.sum(e, axis=1, keepdims=True)
        acc = jnp.dot(e.astype(bf16), new_v, preferred_element_type=f32)
        for i, r in enumerate(olds):
            g = jnp.exp2((tops[:, i : i + 1] - top) * factor)
            total = total + sums[:, i : i + 1] * g
            acc = acc + r[: users * cands, :].astype(f32) * g
        acc_out[...] = acc
        marks_out[...] = jnp.where(iota((users * cands, 128), 1) == 0, top, total)

        send.wait()
        put_rows(hist, base, table_s, flat, place_k, place_v, base_slot, pieces, slots, groups, span)

    return body


def far_kernel(cap, groups, span, scale, parts):
    pieces = cap // 8 // parts
    slots = groups * 8

    def body(
        hist, active, table, ends, xa, xb, w, q, r2, acc_in, marks_in, pk, pv, nk_in, nv_in,
        place_k, place_v, nk, nv, att,
        flat, out_k, out_v, out_a, table_s, sem, in_sem, out_sem, att_sem,
    ):
        factor = scale * LOG2E
        users, cands, width = q.shape
        here = lax.axis_index("pos")
        base = here * span
        base_slot = (1 - here % parts) * (cap // parts)
        send = pltpu.make_async_copy(table, table_s, sem)
        send.start()
        new_k, new_v = project([(xa, 0), (xb, 0)], w, flat, slots)
        send.wait()
        ins = {}
        for u in range(users):
            first, last = bounds(hist, base, table_s, groups, u)
            for b in range(span // STEP):
                lo, hi = b * STEP, (b + 1) * STEP
                edge = (first < hi) & (last > lo) & ((first > lo) | (last < hi))
                copies = [
                    pltpu.make_async_copy(
                        src.at[u, pl.ds(lo, STEP), :], buf.at[u, pl.ds(lo, STEP), :], in_sem.at[i, u, b]
                    )
                    for i, (src, buf) in enumerate(((nk, out_k), (nv, out_v)))
                ]
                ins[u, b] = edge, copies

                @pl.when(edge)
                def _():
                    for copy in copies:
                        copy.start()

        put_rows(hist, base, table_s, flat, place_k, place_v, base_slot, pieces, slots, groups, span)
        pending = []
        for u in range(users):
            first, last = bounds(hist, base, table_s, groups, u)
            for b in range(span // STEP):
                lo, hi = b * STEP, (b + 1) * STEP
                hit = (first < hi) & (last > lo) & (last > first)
                edge, olds = ins[u, b]
                at = iota((STEP, 128), 0) + lo
                copies = [
                    pltpu.make_async_copy(
                        buf.at[u, pl.ds(lo, STEP), :], out.at[u, pl.ds(lo, STEP), :], out_sem.at[i, u, b]
                    )
                    for i, (buf, out) in enumerate(((out_k, nk), (out_v, nv)))
                ]
                pending.append((hit, copies))

                @pl.when(edge)
                def _():
                    for copy in olds:
                        copy.wait()
                    ok = (at >= first) & (at < last)
                    for j in range(width // 128):
                        lanes = slice(j * 128, (j + 1) * 128)
                        for buf, new in ((out_k, place_k), (out_v, place_v)):
                            was = buf[u, lo:hi, lanes].astype(f32)
                            now = new[u, j, GUARD + lo : GUARD + hi, :]
                            buf[u, lo:hi, lanes] = jnp.where(ok, now, was).astype(bf16)

                @pl.when(hit & jnp.logical_not(edge))
                def _():
                    for j in range(width // 128):
                        lanes = slice(j * 128, (j + 1) * 128)
                        for buf, new in ((out_k, place_k), (out_v, place_v)):
                            now = new[u, j, GUARD + lo : GUARD + hi, :]
                            buf[u, lo:hi, lanes] = now.astype(bf16)

                @pl.when(hit)
                def _():
                    for copy in copies:
                        copy.start()

        s = new_scores((ends[0:1, :], ends[8:9, :]), base_slot, pieces, slots, q, new_k)
        tops, sums = old_marks((r2,), users, cands)
        top_one = marks_in[:, 0:1]
        top = jnp.maximum(jnp.max(s, axis=1, keepdims=True), jnp.maximum(top_one, tops))
        g = jnp.exp2((top_one - top) * factor)
        e = jnp.exp2((s - top) * factor)
        total = jnp.sum(e, axis=1, keepdims=True) + marks_in[:, 1:2] * g
        acc = jnp.dot(e.astype(bf16), new_v, preferred_element_type=f32) + acc_in[...] * g
        g = jnp.exp2((tops - top) * factor)
        total = total + sums * g
        acc = acc + r2[: users * cands, :].astype(f32) * g
        acc = acc * (1.0 / total)
        finals = []
        for u in range(users):
            live = active[u].astype(f32)
            out_a[u] = (acc[u * cands : (u + 1) * cands] * live).astype(bf16)
            finals.append(pltpu.make_async_copy(out_a.at[u], att.at[u], att_sem.at[u]))
            finals[-1].start()

        for hit, copies in pending:

            @pl.when(hit)
            def _():
                for copy in copies:
                    copy.wait()

        for copy in finals:
            copy.wait()

    return body


def on_device(
    events, owners, offsets, w_key, w_value, cache_keys, cache_values, hist_len, active, candidates
):
    groups = lax.axis_size("user")
    blocks = lax.axis_size("pos")
    users, span, width = cache_keys.shape
    cands = candidates.shape[1]
    per_event = events.shape[0]
    cap = 2 * per_event // groups
    parts = 2
    scale = width ** (-0.5)
    VM = pl.BlockSpec(memory_space=pltpu.VMEM)
    SM = pl.BlockSpec(memory_space=pltpu.SMEM)
    HB = pl.BlockSpec(memory_space=pltpu.HBM)

    def moved(x, by):
        return lax.ppermute(x, "pos", [(i, (i + by) % blocks) for i in range(blocks)])

    def shape(*dims, dtype=bf16):
        return jax.ShapeDtypeStruct(dims, dtype)

    def grant(mib):
        return pltpu.CompilerParams(vmem_limit_bytes=mib << 20)

    q1 = moved(candidates, 1)
    q3 = moved(candidates, 3)
    q2 = moved(candidates, 2)

    slots = groups * 8
    pieces = cap // 8 // parts
    wide = pieces * ROW + META
    sent = pl.pallas_call(
        route_kernel(cap, groups, parts),
        out_shape=shape(groups, 8, wide),
        in_specs=[HB] * 3,
        out_specs=VM,
        scratch_shapes=[
            pltpu.VMEM((1, per_event), i32),
            pltpu.VMEM((1, per_event), i32),
            pltpu.VMEM(events.shape, bf16),
            pltpu.SemaphoreType.DMA((3,)),
        ],
        compiler_params=grant(60),
        name="route",
    )(owners.reshape(1, -1), offsets.reshape(1, -1), events)
    rows = lax.all_to_all(sent, "user", split_axis=0, concat_axis=0, tiled=True)

    cache = [
        pltpu.VMEM(cache_keys.shape, bf16),
        pltpu.VMEM(cache_values.shape, bf16),
        pltpu.SemaphoreType.DMA((2 * users,)),
    ]
    part = shape(users * cands + 32, width)
    r1, r3 = pl.pallas_call(
        old_kernel(span, scale, 2, False),
        out_shape=[part] * 2,
        in_specs=[SM] + [VM] * 2 + [HB] * 2,
        out_specs=[VM] * 2,
        scratch_shapes=cache,
        compiler_params=grant(52),
        name="olda",
    )(hist_len, q1, q3, cache_keys, cache_values)
    b1 = moved(r1, blocks - 1)
    b3 = moved(r3, blocks - 3)
    r2, r0, w, nk, nv = pl.pallas_call(
        old_kernel(span, scale, 2, True),
        out_shape=[part] * 2 + [shape(width, 2 * width)] + [shape(*cache_keys.shape)] * 2,
        in_specs=[SM] + [VM] * 4 + [HB] * 2,
        out_specs=[VM] * 3 + [HB] * 2,
        scratch_shapes=cache + [pltpu.SemaphoreType.DMA((users, 2))],
        compiler_params=grant(58),
        name="oldb",
    )(hist_len, q2, candidates, w_key, w_value, cache_keys, cache_values)
    b2 = moved(r2, blocks - 2)

    xa = moved(rows[:, :, :ROW], blocks - 1)
    xb = moved(rows[:, :, ROW : 2 * ROW], 1)
    place = (users, width // 128, GUARD + span + 32, 128)
    pk, pv, acc, marks, table, ends = pl.pallas_call(
        near_kernel(cap, groups, span, scale, parts),
        out_shape=[
            shape(*place, dtype=f32),
            shape(*place, dtype=f32),
            shape(users * cands, width, dtype=f32),
            shape(users * cands, 128, dtype=f32),
            shape(groups, META, dtype=i32),
            shape(16, pieces * slots, dtype=i32),
        ],
        in_specs=[SM] + [VM] * 6,
        out_specs=[VM] * 6,
        scratch_shapes=[
            pltpu.VMEM((pieces * slots, 2 * width), f32),
            pltpu.SMEM((groups, META), i32),
            pltpu.SemaphoreType.DMA,
        ],
        compiler_params=grant(30),
        name="near",
    )(hist_len, rows, w, candidates, r0, b1, b3)
    _, _, nk, nv, att = pl.pallas_call(
        far_kernel(cap, groups, span, scale, parts),
        out_shape=[
            shape(*place, dtype=f32),
            shape(*place, dtype=f32),
            shape(*cache_keys.shape),
            shape(*cache_values.shape),
            shape(*candidates.shape),
        ],
        in_specs=[SM] * 2 + [VM] * 11 + [HB] * 2,
        out_specs=[VM] * 2 + [HB] * 3,
        scratch_shapes=[
            pltpu.VMEM((pieces * slots, 2 * width), f32),
            pltpu.VMEM(cache_keys.shape, bf16),
            pltpu.VMEM(cache_values.shape, bf16),
            pltpu.VMEM(candidates.shape, bf16),
            pltpu.SMEM((groups, META), i32),
            pltpu.SemaphoreType.DMA,
            pltpu.SemaphoreType.DMA((2, users, span // STEP)),
            pltpu.SemaphoreType.DMA((2, users, span // STEP)),
            pltpu.SemaphoreType.DMA((users,)),
        ],
        input_output_aliases={11: 0, 12: 1, 13: 2, 14: 3},
        compiler_params=grant(30),
        name="far",
    )(hist_len, active, table, ends, xa, xb, w, candidates, b2, acc, marks, pk, pv, nk, nv)
    return nk, nv, att


def solution(mesh):
    placed = (
        P("user", None),
        P("user"),
        P("user"),
        P(),
        P(),
        P("user", "pos", None),
        P("user", "pos", None),
        P("user"),
        P("user"),
        P("user", "pos", None),
    )

    return jax.shard_map(
        on_device,
        mesh=mesh,
        in_specs=placed,
        out_specs=(P("user", "pos", None), P("user", "pos", None), P("user", "pos", None)),
        check_vma=False,
    )
```

```python
import jax
import jax.numpy as jnp
from jax import lax
from jax.experimental import pallas as pl
from jax.experimental.pallas import tpu as pltpu
from jax.sharding import PartitionSpec as P


NEG = -1e30
LOG2E = 1.4426950408889634
bf16 = jnp.bfloat16
f32 = jnp.float32
i32 = jnp.int32
NT = (((1,), (1,)), ((), ()))
ROW = 256
META = 128
HALF = META // 2
GUARD = 64
STEP = 256


def iota(shape, dim):
    return lax.broadcasted_iota(i32, shape, dim)


def split3(x):
    hi = x.astype(bf16)
    rest = x - hi.astype(f32)
    mid = rest.astype(bf16)
    low = (rest - mid.astype(f32)).astype(bf16)
    return hi, mid, low


def fetch(pairs, sems):
    copies = [pltpu.make_async_copy(a, b, sems.at[i]) for i, (a, b) in enumerate(pairs)]
    for copy in copies:
        copy.start()
    return copies


def route_kernel(cap, groups, parts):
    pieces = cap // 8 // parts

    def body(owners_hbm, offsets_hbm, events_hbm, out, owners, offsets, events, sems):
        loads = fetch(((owners_hbm, owners), (offsets_hbm, offsets), (events_hbm, events)), sems)
        part = lax.axis_index("pos") % parts
        n = owners.shape[1]
        users = 2 * groups
        rows = groups * 8
        at = iota((rows, 1), 0)
        pair = (at // 8) * 2
        loads[0].wait()
        own = owners[...]
        loads[1].wait()
        off = offsets[...]
        who = iota((users, n), 0)
        mine = who == own
        base = jnp.min(jnp.where(mine, off, jnp.int32(1 << 24)), axis=1, keepdims=True)
        count = jnp.sum(jnp.where(mine, 1.0, 0.0), axis=1, keepdims=True).astype(i32)
        each = jnp.broadcast_to(count.astype(bf16), (users, META))
        first = jnp.where(pair == iota((rows, users), 1), 1.0, 0.0).astype(bf16)
        second = jnp.where(pair + 1 == iota((rows, users), 1), 1.0, 0.0).astype(bf16)
        c0 = jnp.dot(first, each, preferred_element_type=f32)
        c1 = jnp.dot(second, each, preferred_element_type=f32)
        both = jnp.where(iota((rows, META), 1) < HALF, c0, c1)
        out[:, :, pieces * ROW :] = both.astype(bf16).reshape(groups, 8, META)
        before = (who == own - 1) & (own % 2 == 1)
        shift = jnp.where(mine, -base, 0) + jnp.where(before, count, 0)
        key = (own // 2) * cap + off + jnp.sum(shift, axis=0, keepdims=True)
        key = key - part * (cap // parts)
        start = (at // 8) * cap + at % 8
        loads[2].wait()
        raw = events[...]
        for c in range(pieces):
            pick = jnp.where(start + 8 * c == key, 1.0, 0.0).astype(bf16)
            got = jnp.dot(pick, raw, preferred_element_type=f32)
            out[:, :, c * ROW : (c + 1) * ROW] = got.astype(bf16).reshape(groups, 8, ROW)

    return body


def old_kernel(span, scale, chunks, keep):
    def body(hist, *refs):
        qs = refs[:chunks]
        refs = refs[chunks:]
        if keep:
            wk, wv, keys_hbm, values_hbm = refs[:4]
            outs = refs[4 : 4 + chunks]
            nk, nv, keys, values, sems, out_sems = refs[4 + chunks :]
        else:
            keys_hbm, values_hbm = refs[:2]
            outs = refs[2 : 2 + chunks]
            keys, values, sems = refs[2 + chunks :]
        users, cands, width = qs[0].shape
        loads = fetch(
            [p for u in range(users) for p in ((keys_hbm.at[u], keys.at[u]), (values_hbm.at[u], values.at[u]))],
            sems,
        )
        factor = scale * LOG2E
        base = lax.axis_index("pos") * span
        if keep:
            tail = users * cands + 32
            outs[0][tail : tail + width, :] = wk[...]
            outs[0][tail + width :, :] = wv[...]
        stores = []
        for i, (q, r) in enumerate(zip(qs, outs)):
            marks = []
            for u in range(users):
                if i == 0:
                    loads[2 * u].wait()
                    loads[2 * u + 1].wait()
                    if keep:
                        stores += fetch(
                            ((keys.at[u], nk.at[u]), (values.at[u], nv.at[u])), out_sems.at[u]
                        )
                s = lax.dot_general(q[u], keys[u], NT, preferred_element_type=f32)
                s = jnp.where(iota((1, span), 1) < hist[u] - base, s, NEG)
                top = jnp.max(s, axis=1, keepdims=True)
                e = jnp.exp2((s - top) * factor)
                total = jnp.sum(e, axis=1, keepdims=True)
                part = jnp.dot(e.astype(bf16), values[u], preferred_element_type=f32)
                r[u * cands : (u + 1) * cands, :] = part.astype(bf16)
                marks += [top, total]
            lane = iota((cands, 128), 1)
            mat = jnp.zeros((cands, 128), f32)
            for k, v in enumerate(marks):
                mat = jnp.where(lane == k, v, mat)
            rows = mat.T[:8, :]
            hi, mid, low = split3(rows)
            r[users * cands : users * cands + 32, :] = jnp.concatenate(
                [hi, mid, low, jnp.zeros_like(hi)], axis=0
            )
        for copy in stores:
            copy.wait()

    return body


def tables(meta, groups, slots):
    src = iota((groups, slots), 0)
    col = iota((groups, slots), 1)
    lead = (col % 8) == 0
    earlier = jnp.where(lead & (col // 8 < src), 1.0, 0.0).astype(bf16)
    same = jnp.where(lead & (col // 8 == src), 1.0, 0.0).astype(bf16)
    begin = jnp.dot(earlier, meta, preferred_element_type=f32)
    here = jnp.dot(same, meta, preferred_element_type=f32)
    lane = iota((groups, META), 1)
    return jnp.where(lane % 2 == 0, begin, here).astype(i32)


def project(refs, w, flat, slots):
    ys = []
    for c, (ref, lane) in enumerate(refs):
        x = ref[:, :, lane : lane + ROW].reshape(slots, ROW)
        width = w.shape[1]
        pair = []
        for i in range(2):
            top = w.shape[0] - (2 - i) * ROW
            y = jnp.dot(x, w[top : top + ROW, :], preferred_element_type=f32).astype(bf16)
            flat[c * slots : (c + 1) * slots, i * width : (i + 1) * width] = y.astype(f32)
            pair.append(y)
        ys.append(pair)
    keys = jnp.concatenate([y[0] for y in ys], axis=0)
    values = jnp.concatenate([y[1] for y in ys], axis=0)
    return keys, values


def put_rows(hist, base, table_s, flat, place_k, place_v, base_slot, pieces, slots, groups, span):
    users = place_k.shape[0]
    tiles = place_k.shape[1]
    most = GUARD + span

    def put(s, carry):
        n0 = table_s[s, 1]
        for u in range(users):
            n = table_s[s, u * HALF + 1]
            d = hist[u] - base + table_s[s, u * HALF]
            a = 0 if u == 0 else n0
            for c in range(pieces):
                slot = iota((8, 128), 0) + (8 * c + base_slot)
                ok = (slot >= a) & (slot < a + n)
                to = jnp.clip(d - a + (8 * c + base_slot + GUARD), 0, most)
                from_row = pl.multiple_of(c * slots + s * 8, 8)
                for j in range(tiles):
                    for dst, o in ((place_k, 0), (place_v, tiles * 128)):
                        v = flat[pl.ds(from_row, 8), o + j * 128 : o + (j + 1) * 128]
                        pltpu.store(dst.at[u, j, pl.ds(to, 8), :], v, mask=ok)
        return carry

    lax.fori_loop(0, groups, put, 0, unroll=8)


def slot_ends(meta, pieces):
    mt = meta.astype(f32).T
    c0 = mt[0:1, :].astype(i32)
    c1 = mt[HALF : HALF + 1, :].astype(i32)
    end0 = jnp.concatenate([c0] * pieces, axis=1)
    end1 = jnp.concatenate([c0 + c1] * pieces, axis=1)
    return end0, end1


def new_scores(ends, base_slot, pieces, slots, q, keys):
    users, cands, width = q.shape
    end0, end1 = ends
    at = iota((1, slots), 1) % 8 + base_slot
    slot = jnp.concatenate([at + 8 * c for c in range(pieces)], axis=1)
    s = lax.dot_general(
        q[...].reshape(users * cands, width), keys, NT, preferred_element_type=f32
    )
    return jnp.concatenate(
        [
            jnp.where(slot < end0, s[:cands], NEG),
            jnp.where((slot >= end0) & (slot < end1), s[cands:], NEG),
        ],
        axis=0,
    )


def old_marks(olds, users, cands):
    marks = []
    for r in olds:
        m = r[users * cands : users * cands + 32, :].astype(f32)
        marks.append(m[0:8] + m[8:16] + m[16:24])
    count = len(olds)
    stack = jnp.concatenate(
        [m[k : k + 1] for k in range(2 * users) for m in marks]
        + [jnp.zeros((128 - 2 * users * count, cands), f32)],
        axis=0,
    ).T
    per = 2 * count
    tops = jnp.concatenate([stack[:, per * u : per * u + count] for u in range(users)], axis=0)
    sums = jnp.concatenate(
        [stack[:, per * u + count : per * u + per] for u in range(users)], axis=0
    )
    return tops, sums


def bounds(hist, base, table_s, groups, u):
    first = hist[u] - base
    count = table_s[groups - 1, u * HALF] + table_s[groups - 1, u * HALF + 1]
    return first, first + count


def near_kernel(cap, groups, span, scale, parts):
    pieces = cap // 8 // parts
    slots = groups * 8

    def body(
        hist, rows, q, r0, r1, r2, r3,
        place_k, place_v, acc_out, marks_out, table, ends_out,
        flat, table_s, sem,
    ):
        factor = scale * LOG2E
        users, cands, _ = q.shape
        here = lax.axis_index("pos")
        base = here * span
        base_slot = (here % parts) * (cap // parts)
        meta = rows[:, :, pieces * ROW :].reshape(slots, META)
        table[...] = tables(meta, groups, slots)
        send = pltpu.make_async_copy(table, table_s, sem)
        send.start()
        new_k, new_v = project([(rows, c * ROW) for c in range(pieces)], r0, flat, slots)
        ends = slot_ends(meta, pieces)
        for i, row in enumerate(ends):
            ends_out[8 * i : 8 * i + 8, :] = jnp.broadcast_to(row, (8, pieces * slots))
        s = new_scores(ends, base_slot, pieces, slots, q, new_k)
        olds = (r0, r1, r2, r3)
        tops, sums = old_marks(olds, users, cands)
        top = jnp.maximum(
            jnp.max(s, axis=1, keepdims=True), jnp.max(tops, axis=1, keepdims=True)
        )
        e = jnp.exp2((s - top) * factor)
        total = jnp.sum(e, axis=1, keepdims=True)
        acc = jnp.dot(e.astype(bf16), new_v, preferred_element_type=f32)
        for i, r in enumerate(olds):
            g = jnp.exp2((tops[:, i : i + 1] - top) * factor)
            total = total + sums[:, i : i + 1] * g
            acc = acc + r[: users * cands, :].astype(f32) * g
        acc_out[...] = acc
        marks_out[...] = jnp.where(iota((users * cands, 128), 1) == 0, top, total)

        send.wait()
        put_rows(hist, base, table_s, flat, place_k, place_v, base_slot, pieces, slots, groups, span)

    return body


def far_kernel(cap, groups, span, scale, parts):
    pieces = cap // 8 // parts
    slots = groups * 8

    def body(
        hist, active, table, ends, xa, xb, w, q, acc_in, marks_in, pk, pv, nk_in, nv_in,
        place_k, place_v, nk, nv, att,
        flat, out_k, out_v, out_a, table_s, sem, in_sem, out_sem, att_sem,
    ):
        factor = scale * LOG2E
        users, cands, width = q.shape
        here = lax.axis_index("pos")
        base = here * span
        base_slot = (1 - here % parts) * (cap // parts)
        send = pltpu.make_async_copy(table, table_s, sem)
        send.start()
        new_k, new_v = project([(xa, 0), (xb, 0)], w, flat, slots)
        s = new_scores((ends[0:1, :], ends[8:9, :]), base_slot, pieces, slots, q, new_k)
        top_one = marks_in[:, 0:1]
        top = jnp.maximum(jnp.max(s, axis=1, keepdims=True), top_one)
        g = jnp.exp2((top_one - top) * factor)
        e = jnp.exp2((s - top) * factor)
        total = jnp.sum(e, axis=1, keepdims=True) + marks_in[:, 1:2] * g
        acc = jnp.dot(e.astype(bf16), new_v, preferred_element_type=f32) + acc_in[...] * g
        acc = acc * (1.0 / total)
        finals = []
        for u in range(users):
            live = active[u].astype(f32)
            out_a[u] = (acc[u * cands : (u + 1) * cands] * live).astype(bf16)
            finals.append(pltpu.make_async_copy(out_a.at[u], att.at[u], att_sem.at[u]))
            finals[-1].start()

        send.wait()
        ins = {}
        for u in range(users):
            first, last = bounds(hist, base, table_s, groups, u)
            for b in range(span // STEP):
                lo, hi = b * STEP, (b + 1) * STEP
                edge = (first < hi) & (last > lo) & ((first > lo) | (last < hi))
                copies = [
                    pltpu.make_async_copy(
                        src.at[u, pl.ds(lo, STEP), :], buf.at[u, pl.ds(lo, STEP), :], in_sem.at[i, u, b]
                    )
                    for i, (src, buf) in enumerate(((nk, out_k), (nv, out_v)))
                ]
                ins[u, b] = edge, copies

                @pl.when(edge)
                def _():
                    for copy in copies:
                        copy.start()

        put_rows(hist, base, table_s, flat, place_k, place_v, base_slot, pieces, slots, groups, span)
        pending = []
        for u in range(users):
            first, last = bounds(hist, base, table_s, groups, u)
            for b in range(span // STEP):
                lo, hi = b * STEP, (b + 1) * STEP
                hit = (first < hi) & (last > lo) & (last > first)
                edge, olds = ins[u, b]
                at = iota((STEP, 128), 0) + lo
                copies = [
                    pltpu.make_async_copy(
                        buf.at[u, pl.ds(lo, STEP), :], out.at[u, pl.ds(lo, STEP), :], out_sem.at[i, u, b]
                    )
                    for i, (buf, out) in enumerate(((out_k, nk), (out_v, nv)))
                ]
                pending.append((hit, copies))

                @pl.when(edge)
                def _():
                    for copy in olds:
                        copy.wait()
                    ok = (at >= first) & (at < last)
                    for j in range(width // 128):
                        lanes = slice(j * 128, (j + 1) * 128)
                        for buf, new in ((out_k, place_k), (out_v, place_v)):
                            was = buf[u, lo:hi, lanes].astype(f32)
                            now = new[u, j, GUARD + lo : GUARD + hi, :]
                            buf[u, lo:hi, lanes] = jnp.where(ok, now, was).astype(bf16)

                @pl.when(hit & jnp.logical_not(edge))
                def _():
                    for j in range(width // 128):
                        lanes = slice(j * 128, (j + 1) * 128)
                        for buf, new in ((out_k, place_k), (out_v, place_v)):
                            now = new[u, j, GUARD + lo : GUARD + hi, :]
                            buf[u, lo:hi, lanes] = now.astype(bf16)

                @pl.when(hit)
                def _():
                    for copy in copies:
                        copy.start()

        for hit, copies in pending:

            @pl.when(hit)
            def _():
                for copy in copies:
                    copy.wait()

        for copy in finals:
            copy.wait()

    return body


def on_device(
    events, owners, offsets, w_key, w_value, cache_keys, cache_values, hist_len, active, candidates
):
    groups = lax.axis_size("user")
    blocks = lax.axis_size("pos")
    users, span, width = cache_keys.shape
    cands = candidates.shape[1]
    per_event = events.shape[0]
    cap = 2 * per_event // groups
    parts = 2
    scale = width ** (-0.5)
    VM = pl.BlockSpec(memory_space=pltpu.VMEM)
    SM = pl.BlockSpec(memory_space=pltpu.SMEM)
    HB = pl.BlockSpec(memory_space=pltpu.HBM)

    def moved(x, by):
        return lax.ppermute(x, "pos", [(i, (i + by) % blocks) for i in range(blocks)])

    def shape(*dims, dtype=bf16):
        return jax.ShapeDtypeStruct(dims, dtype)

    def grant(mib):
        return pltpu.CompilerParams(vmem_limit_bytes=mib << 20)

    q1 = moved(candidates, 1)
    q3 = moved(candidates, 3)
    q2 = moved(candidates, 2)

    slots = groups * 8
    pieces = cap // 8 // parts
    wide = pieces * ROW + META
    sent = pl.pallas_call(
        route_kernel(cap, groups, parts),
        out_shape=shape(groups, 8, wide),
        in_specs=[HB] * 3,
        out_specs=VM,
        scratch_shapes=[
            pltpu.VMEM((1, per_event), i32),
            pltpu.VMEM((1, per_event), i32),
            pltpu.VMEM(events.shape, bf16),
            pltpu.SemaphoreType.DMA((3,)),
        ],
        compiler_params=grant(60),
        name="route",
    )(owners.reshape(1, -1), offsets.reshape(1, -1), events)
    rows = lax.all_to_all(sent, "user", split_axis=0, concat_axis=0, tiled=True)

    cache = [
        pltpu.VMEM(cache_keys.shape, bf16),
        pltpu.VMEM(cache_values.shape, bf16),
        pltpu.SemaphoreType.DMA((2 * users,)),
    ]
    part = shape(users * cands + 32, width)
    (r2,) = pl.pallas_call(
        old_kernel(span, scale, 1, False),
        out_shape=[part],
        in_specs=[SM] + [VM] + [HB] * 2,
        out_specs=[VM],
        scratch_shapes=cache,
        compiler_params=grant(52),
        name="olda",
    )(hist_len, q2, cache_keys, cache_values)
    b2 = moved(r2, blocks - 2)
    r1, r3 = pl.pallas_call(
        old_kernel(span, scale, 2, False),
        out_shape=[part] * 2,
        in_specs=[SM] + [VM] * 2 + [HB] * 2,
        out_specs=[VM] * 2,
        scratch_shapes=cache,
        compiler_params=grant(52),
        name="oldb",
    )(hist_len, q1, q3, cache_keys, cache_values)
    b1 = moved(r1, blocks - 1)
    b3 = moved(r3, blocks - 3)
    r0, nk, nv = pl.pallas_call(
        old_kernel(span, scale, 1, True),
        out_shape=[shape(users * cands + 32 + 2 * ROW, width)] + [shape(*cache_keys.shape)] * 2,
        in_specs=[SM] + [VM] * 3 + [HB] * 2,
        out_specs=[VM] + [HB] * 2,
        scratch_shapes=cache + [pltpu.SemaphoreType.DMA((users, 2))],
        compiler_params=grant(58),
        name="oldc",
    )(hist_len, candidates, w_key, w_value, cache_keys, cache_values)

    xa = moved(rows[:, :, :ROW], blocks - 1)
    xb = moved(rows[:, :, ROW : 2 * ROW], 1)
    place = (users, width // 128, GUARD + span + 32, 128)
    pk, pv, acc, marks, table, ends = pl.pallas_call(
        near_kernel(cap, groups, span, scale, parts),
        out_shape=[
            shape(*place, dtype=f32),
            shape(*place, dtype=f32),
            shape(users * cands, width, dtype=f32),
            shape(users * cands, 128, dtype=f32),
            shape(groups, META, dtype=i32),
            shape(16, pieces * slots, dtype=i32),
        ],
        in_specs=[SM] + [VM] * 6,
        out_specs=[VM] * 6,
        scratch_shapes=[
            pltpu.VMEM((pieces * slots, 2 * width), f32),
            pltpu.SMEM((groups, META), i32),
            pltpu.SemaphoreType.DMA,
        ],
        compiler_params=grant(30),
        name="near",
    )(hist_len, rows, candidates, r0, b1, b2, b3)
    _, _, nk, nv, att = pl.pallas_call(
        far_kernel(cap, groups, span, scale, parts),
        out_shape=[
            shape(*place, dtype=f32),
            shape(*place, dtype=f32),
            shape(*cache_keys.shape),
            shape(*cache_values.shape),
            shape(*candidates.shape),
        ],
        in_specs=[SM] * 2 + [VM] * 10 + [HB] * 2,
        out_specs=[VM] * 2 + [HB] * 3,
        scratch_shapes=[
            pltpu.VMEM((pieces * slots, 2 * width), f32),
            pltpu.VMEM(cache_keys.shape, bf16),
            pltpu.VMEM(cache_values.shape, bf16),
            pltpu.VMEM(candidates.shape, bf16),
            pltpu.SMEM((groups, META), i32),
            pltpu.SemaphoreType.DMA,
            pltpu.SemaphoreType.DMA((2, users, span // STEP)),
            pltpu.SemaphoreType.DMA((2, users, span // STEP)),
            pltpu.SemaphoreType.DMA((users,)),
        ],
        input_output_aliases={10: 0, 11: 1, 12: 2, 13: 3},
        compiler_params=grant(30),
        name="far",
    )(hist_len, active, table, ends, xa, xb, r0, candidates, acc, marks, pk, pv, nk, nv)
    return nk, nv, att


def solution(mesh):
    placed = (
        P("user", None),
        P("user"),
        P("user"),
        P(),
        P(),
        P("user", "pos", None),
        P("user", "pos", None),
        P("user"),
        P("user"),
        P("user", "pos", None),
    )

    return jax.shard_map(
        on_device,
        mesh=mesh,
        in_specs=placed,
        out_specs=(P("user", "pos", None), P("user", "pos", None), P("user", "pos", None)),
        check_vma=False,
    )
```
